32 devices in a mesh: gx: 2 (over x), gy: 4 (over z), gz: 4 (over y, core).
Axes of the slice: x: 2, y: 2, z: 4, core: 2. Of those that a mesh axis runs over, the one named last changes fastest.
Arguments:
- vectors: float32 [3, 12, 24, 24, 128], P(None, 'gx', 'gy', 'gz'), may hold values from -6 to 6
- orient_flip: int32 [4, 8, 1152], P('gx', 'gy', 'gz'), may hold values from 0 to 1
- reluctivity: float32 [4, 8, 512], P('gx', 'gy', 'gz'), may hold values from 0.05 to 0.5
- conductivity: float32 [4, 8, 512], P('gx', 'gy', 'gz'), may hold values from 1 to 10
Outputs:
- out_x: float32 [12, 28, 28, 128], P('gx', 'gy', 'gz')
- out_y: float32 [14, 24, 28, 128], P('gx', 'gy', 'gz')
- out_z: float32 [14, 28, 24, 128], P('gx', 'gy', 'gz')
The draws below stay inside these ranges and needn't reach their ends.
Inputs may be any that keep to these rules, and one draw needn't show every extreme that they name: `orient_flip`: 1 reverses the orientation of that degree of freedom in that element, 0 keeps it.
All inputs are finite; a program needn't handle non-finite values.
Results may differ from the reference program's by a relative error of at most 0.00007.
Values sent between devices are 32-bit elements; how exact they have to be, the bound alone decides.
No kernel may reach another device: no remote copies, remote signals or barrier semaphores. Data moves between devices by JAX's collectives and lax.ppermute only.
A program may use at most 64 MiB of HBM per device.

```python
import math
import jax
import jax.numpy as jnp
import numpy as np
from jax import lax

ORDER = 3
QUAD = 4
VECS = 128
NX = 4
NY = 8
NZ = 8
ELEM_DOFS = 144
QPTS = 64
N_GX = 2
N_GY = 4
N_GZ = 4


def touch_ends(entries, key, low, high):
    place = [jax.random.randint(jax.random.fold_in(key, axis), (), 0, length) for axis, length in enumerate(entries.shape)]
    widest = entries.shape.index(max(entries.shape))
    neighbour = place[:widest] + [(place[widest] + 1) % entries.shape[widest]] + place[widest + 1:]
    return entries.at[tuple(place)].set(low).at[tuple(neighbour)].set(high)


def levels(key, shape, shards, least, largest):
    gain, own = 1.0, jax.random.fold_in(key, 6)
    for axis_at, parts in shards:
        heights = jnp.exp(jax.random.uniform(jax.random.fold_in(own, axis_at), (parts,), jnp.float32, least / len(shards), largest / len(shards)))
        gain = gain * jnp.repeat(heights, shape[axis_at] // parts).reshape([-1 if axis == axis_at else 1 for axis in range(len(shape))])
    return gain


def scatter_about(own_key, shape, scale, most, pieces=(), kind=jnp.bfloat16):
    entries = jax.random.normal(own_key, shape, jnp.float32) * scale
    if len(pieces) > 0:
        entries = levels(own_key, shape, pieces, -0.22, 0.18) * entries
    return jnp.clip(entries, min=-most, max=most).astype(kind)


def setup_inputs(seed: int = 0) -> dict:
    key_of = jax.random.split(jax.random.key(seed), 5)
    vectors = scatter_about(key_of[0], (3, NX * ORDER, NY * ORDER, NZ * ORDER, VECS), 1.0, 6.0, ((1, 2), (2, 4), (3, 4)), jnp.float32)
    orient_flip = touch_ends(jax.random.randint(key_of[1], (NX, NY, NZ * ELEM_DOFS), 0, 2), jax.random.fold_in(key_of[1], 1), 0, 1).astype(jnp.int32)
    reluctivity = jnp.clip(jnp.exp(math.log(0.5) - 2.3025851 * jax.random.uniform(key_of[2], (NX, NY, NZ * QPTS), jnp.float32) ** levels(key_of[2], (NX, NY, NZ * QPTS), ((0, 2), (1, 4), (2, 4)), -0.2, 0.2)), 0.05, 0.5)
    conductivity = jnp.clip(jnp.exp(math.log(10.0) - 2.3025851 * jax.random.uniform(key_of[3], (NX, NY, NZ * QPTS), jnp.float32) ** levels(key_of[3], (NX, NY, NZ * QPTS), ((0, 2), (1, 4), (2, 4)), -0.2, 0.2)), 1.0, 10.0)
    return {"vectors": vectors, "orient_flip": orient_flip, "reluctivity": reluctivity, "conductivity": conductivity}


def lagrange(points_at, evaluate_at):
    amount = len(points_at)
    values = np.ones((len(evaluate_at), amount))
    slopes = np.zeros((len(evaluate_at), amount))
    for which in range(amount):
        for column in range(amount):
            if column != which:
                factor = (evaluate_at - points_at[column]) / (points_at[which] - points_at[column])
                slopes[:, which] = slopes[:, which] * factor + values[:, which] / (points_at[which] - points_at[column])
                values[:, which] = values[:, which] * factor
    return (values, slopes)

def basis_tables():
    lobatto = np.array([0.0, (1 - 5 ** (-0.5)) / 2, (1 + 5 ** (-0.5)) / 2, 1.0])
    gauss_open = np.array([(1 - 0.6 ** 0.5) / 2, 0.5, (1 + 0.6 ** 0.5) / 2])
    inner_pt = (3.0 / 7 - 2.0 / 7 * (6.0 / 5) ** 0.5) ** 0.5
    outer_pt = (3.0 / 7 + 2.0 / 7 * (6.0 / 5) ** 0.5) ** 0.5
    inner_wt = (18 + 30 ** 0.5) / 36
    outer_wt = (18 - 30 ** 0.5) / 36
    quad_points = (1 + np.array([-outer_pt, -inner_pt, inner_pt, outer_pt])) / 2
    quad_weight = np.array([outer_wt, inner_wt, inner_wt, outer_wt]) / 2
    closed, slopes = lagrange(lobatto, quad_points)
    opened, unused_slopes = lagrange(gauss_open, quad_points)
    weight_cube = quad_weight[:, None, None, None, None] * quad_weight[None, :, None, None, None] * quad_weight[None, None, :, None, None]
    return (jnp.asarray(closed, dtype=jnp.float32), jnp.asarray(slopes, dtype=jnp.float32), jnp.asarray(opened, dtype=jnp.float32), jnp.asarray(weight_cube, dtype=jnp.float32))

def contract(tensor, first_mat, second_mat, third_mat):
    section_one = jnp.einsum('qa,abcef->qbcef', first_mat, tensor, precision=lax.Precision.HIGHEST)
    section_two = jnp.einsum('rb,qbcef->qrcef', second_mat, section_one, precision=lax.Precision.HIGHEST)
    return jnp.einsum('sc,qrcef->qrsef', third_mat, section_two, precision=lax.Precision.HIGHEST)

def evaluate(elem_x, elem_y, elem_z, closed, slopes, opened):
    u_x = contract(elem_x, opened, closed, closed)
    u_y = contract(elem_y, closed, opened, closed)
    u_z = contract(elem_z, closed, closed, opened)
    deriv_xy = contract(elem_x, opened, slopes, closed)
    deriv_xz = contract(elem_x, opened, closed, slopes)
    deriv_yx = contract(elem_y, slopes, opened, closed)
    deriv_yz = contract(elem_y, closed, opened, slopes)
    deriv_zx = contract(elem_z, slopes, closed, opened)
    deriv_zy = contract(elem_z, closed, slopes, opened)
    return (u_x, u_y, u_z, deriv_zy - deriv_yz, deriv_xz - deriv_zx, deriv_yx - deriv_xy)

def windows(array, axis, amount, open_dim):
    dims_now = array.shape
    if open_dim:
        split = array.reshape(dims_now[:axis] + (amount, ORDER) + dims_now[axis + 1:])
        return jnp.swapaxes(split, axis, axis + 1)
    reach = ORDER * (amount - 1) + 1
    return jnp.stack([lax.slice_in_dim(array, offset, offset + reach, ORDER, axis) for offset in range(ORDER + 1)], axis=axis)

def collect(array, open_axis, counts):
    result = array
    for axis in range(3):
        result = windows(result, 2 * axis, counts[axis], axis == open_axis)
    dims_now = result.shape
    result = jnp.transpose(result, (0, 2, 4, 1, 3, 5, 6))
    return result.reshape(dims_now[0], dims_now[2], dims_now[4], counts[0] * counts[1] * counts[2], dims_now[6])

def element_data(orient_flip, reluctivity, conductivity, elements):
    flip_float = orient_flip.reshape(elements, ELEM_DOFS).T.astype(jnp.float32)
    sign_all = 1.0 - 2.0 * flip_float
    per_comp = ORDER * (ORDER + 1) * (ORDER + 1)
    sign_x = sign_all[:per_comp].reshape(ORDER, ORDER + 1, ORDER + 1, elements, 1)
    sign_y = sign_all[per_comp:2 * per_comp].reshape(ORDER + 1, ORDER, ORDER + 1, elements, 1)
    sign_z = sign_all[2 * per_comp:].reshape(ORDER + 1, ORDER + 1, ORDER, elements, 1)
    reluct = reluctivity.reshape(elements, QPTS).T.reshape(QUAD, QUAD, QUAD, elements, 1)
    conduct = conductivity.reshape(elements, QPTS).T.reshape(QUAD, QUAD, QUAD, elements, 1)
    return (sign_x, sign_y, sign_z, reluct, conduct)

def element_apply(lvec_x, lvec_y, lvec_z, data, counts):

    def gather_all(part_x, part_y, part_z):
        return (collect(part_x, 0, counts), collect(part_y, 1, counts), collect(part_z, 2, counts))
    elems, scatter_back = jax.vjp(gather_all, lvec_x, lvec_y, lvec_z)
    sign_x, sign_y, sign_z, reluct, conduct = data
    closed, slopes, opened, weight_cube = basis_tables()

    def forward(part_x, part_y, part_z):
        return evaluate(part_x, part_y, part_z, closed, slopes, opened)
    quads, pullback = jax.vjp(forward, elems[0] * sign_x, elems[1] * sign_y, elems[2] * sign_z)
    mass_scale = weight_cube * conduct
    curl_scale = weight_cube * reluct
    cotangent = (mass_scale * quads[0], mass_scale * quads[1], mass_scale * quads[2], curl_scale * quads[3], curl_scale * quads[4], curl_scale * quads[5])
    grads = pullback(cotangent)
    return scatter_back((grads[0] * sign_x, grads[1] * sign_y, grads[2] * sign_z))

def extend(array, axes):
    for axis in axes:
        array = jnp.concatenate([array, lax.slice_in_dim(array, 0, 1, 1, axis)], axis)
    return array

def fold_back(array, axes):
    for axis in axes:
        total_len = array.shape[axis]
        head_sum = lax.slice_in_dim(array, 0, 1, 1, axis) + lax.slice_in_dim(array, total_len - 1, total_len, 1, axis)
        array = jnp.concatenate([head_sum, lax.slice_in_dim(array, 1, total_len - 1, 1, axis)], axis)
    return array

def spread(array, axis, blocks):
    dims_now = array.shape
    block_len = dims_now[axis] // blocks
    split = array.reshape(dims_now[:axis] + (blocks, block_len) + dims_now[axis + 1:])
    following = jnp.roll(lax.slice_in_dim(split, 0, 1, 1, axis + 1), -1, axis)
    joined = jnp.concatenate([split, following], axis + 1)
    return joined.reshape(dims_now[:axis] + (blocks * (block_len + 1),) + dims_now[axis + 1:])

def reference(vectors, orient_flip, reluctivity, conductivity):
    data = element_data(orient_flip, reluctivity, conductivity, NX * NY * NZ)
    group = math.gcd(VECS, 2)
    dims_now = vectors.shape
    grouped = jnp.moveaxis(vectors.reshape(dims_now[:4] + (VECS // group, group)), 4, 0)

    def apply_whole(single):
        results = element_apply(extend(single[0], (1, 2)), extend(single[1], (0, 2)), extend(single[2], (0, 1)), data, (NX, NY, NZ))
        own_x = fold_back(results[0], (1, 2))
        own_y = fold_back(results[1], (0, 2))
        own_z = fold_back(results[2], (0, 1))
        return (spread(spread(own_x, 1, N_GY), 2, N_GZ), spread(spread(own_y, 0, N_GX), 2, N_GZ), spread(spread(own_z, 0, N_GX), 1, N_GY))
    parts_x, parts_y, parts_z = lax.map(apply_whole, grouped)

    def unite(stacked):
        moved = jnp.moveaxis(stacked, 0, 3)
        shape_now = moved.shape
        return moved.reshape(shape_now[:3] + (VECS,))
    return (unite(parts_x), unite(parts_y), unite(parts_z))
```

```python
import functools

import jax
import jax.numpy as jnp
import numpy as np
from jax import lax
from jax.experimental import pallas as pl
from jax.experimental.pallas import tpu as pltpu
from jax.sharding import PartitionSpec as P

ORDER = 3
QUAD = 4
ELEM_DOFS = 144
QPTS = 64
AXES = ("gx", "gy", "gz")
F32 = jnp.float32
BF16 = jnp.bfloat16


def lagrange(points_at, evaluate_at):
    amount = len(points_at)
    values = np.ones((len(evaluate_at), amount))
    slopes = np.zeros((len(evaluate_at), amount))
    for which in range(amount):
        for column in range(amount):
            if column != which:
                factor = (evaluate_at - points_at[column]) / (points_at[which] - points_at[column])
                slopes[:, which] = slopes[:, which] * factor + values[:, which] / (
                    points_at[which] - points_at[column]
                )
                values[:, which] = values[:, which] * factor
    return (values, slopes)


def rows_of(comp):
    shape = [ORDER + 1] * 3
    shape[comp] = ORDER
    return shape


STARTS = (0, 48, 96)
PADDED = 160


def element_tables():
    lobatto = np.array([0.0, (1 - 5 ** (-0.5)) / 2, (1 + 5 ** (-0.5)) / 2, 1.0])
    gauss_open = np.array([(1 - 0.6**0.5) / 2, 0.5, (1 + 0.6**0.5) / 2])
    inner_pt = (3.0 / 7 - 2.0 / 7 * (6.0 / 5) ** 0.5) ** 0.5
    outer_pt = (3.0 / 7 + 2.0 / 7 * (6.0 / 5) ** 0.5) ** 0.5
    inner_wt = (18 + 30**0.5) / 36
    outer_wt = (18 - 30**0.5) / 36
    quad_points = (1 + np.array([-outer_pt, -inner_pt, inner_pt, outer_pt])) / 2
    quad_weight = np.array([outer_wt, inner_wt, inner_wt, outer_wt]) / 2
    closed, slopes = lagrange(lobatto, quad_points)
    opened, _ = lagrange(gauss_open, quad_points)
    weight = np.einsum("i,j,k->ijk", quad_weight, quad_weight, quad_weight).reshape(-1)

    def table(comp, deriv=None):
        mats = [opened if d == comp else (slopes if d == deriv else closed) for d in range(3)]
        return np.einsum("qa,rb,sc->qrsabc", *mats).reshape(QPTS, -1)

    full = np.zeros((6, QPTS, 3, 48))
    for comp in range(3):
        full[comp, :, comp] = table(comp)
    for out in range(3):
        first, second = (out + 1) % 3, (out + 2) % 3
        full[3 + out, :, second] += table(second, first)
        full[3 + out, :, first] -= table(first, second)
    full = full.reshape(6 * QPTS, ELEM_DOFS)
    place = np.zeros((ELEM_DOFS, PADDED))
    for comp in range(3):
        shape = rows_of(comp)
        for d in range(48):
            a, b, c = np.unravel_index(d, shape)
            place[48 * comp + d, STARTS[comp] + (a * shape[1] + b) * 4 + c] = 1
    return full @ place, np.tile(weight, 6), place


def split(x):
    hi = x.astype(BF16)
    return hi, (x - hi.astype(F32)).astype(BF16)


def dot(a, b):
    return jnp.dot(a, b, preferred_element_type=F32)


def form_kernel(counts, wt_ref, rhs_ref, place_ref, placet_ref, flip_ref, rel_ref, con_ref, hi_ref, lo_ref):
    count_x, count_y, count_z = counts
    lanes = ELEM_DOFS * count_z
    ones = jnp.ones((lanes, PADDED), BF16)
    for i in range(count_x):
        for j in range(count_y):
            sign = 1.0 - 2.0 * flip_ref[i, j : j + 1, :].astype(F32)
            con_all = con_ref[i, j : j + 1, :]
            rel_all = rel_ref[i, j : j + 1, :]
            for k in range(count_z):
                e = (i * count_y + j) * count_z + k
                con = con_all[:, QPTS * k : QPTS * (k + 1)]
                rel = rel_all[:, QPTS * k : QPTS * (k + 1)]
                scale = jnp.concatenate([con, con, con, rel, rel, rel], axis=1)
                hi, lo = split(wt_ref[...] * scale)
                mat = dot(jnp.concatenate([hi, hi, lo], axis=1), rhs_ref[...])
                row = dot(jnp.broadcast_to(sign, (8, lanes)).astype(BF16), place_ref[k])[0:1]
                col = dot((placet_ref[k] * sign).astype(BF16), ones)
                hi, lo = split(mat * row * col)
                hi_ref[e] = hi
                lo_ref[e] = lo


def pack_kernel(vec_ref, x_ref, y_ref, z_ref, xy_ref, xz_ref, yz_ref):
    x_ref[0] = vec_ref[1, 0]
    x_ref[1] = vec_ref[2, 0]
    y_ref[0] = vec_ref[0, :, 0]
    y_ref[1] = vec_ref[2, :, 0]
    z_ref[0] = vec_ref[0, :, :, 0]
    z_ref[1] = vec_ref[1, :, :, 0]
    xy_ref[...] = vec_ref[2, 0, 0]
    xz_ref[...] = vec_ref[1, 0, :, 0]
    yz_ref[...] = vec_ref[0, :, 0, 0]


def sides(dims):
    out = []
    for first in range(3):
        for up in (0, 1):
            key = [0, 0, 0]
            key[first] = 2 * up - 1
            out.append(tuple(key))
    for first in range(3):
        for second in range(first + 1, 3):
            for up in (0, 1):
                for up2 in (0, 1):
                    key = [0, 0, 0]
                    key[first] = 2 * up - 1
                    key[second] = 2 * up2 - 1
                    out.append(tuple(key))
    return out


def message_groups(dims):
    groups = {}
    for key in sides(dims):
        target = tuple(k % d for k, d in zip(key, dims))
        groups.setdefault(target, []).append(key)
    return groups


def plane_index(key, own, sizes):
    return tuple((0 if k < 0 else s) if k else slice(None) for k, s in zip(key, sizes))


def plane_items(key):
    return [c for c in range(3) if not key[c]] if sum(map(abs, key)) == 1 else [key.index(0)]


def region_shape(comp, sizes):
    return tuple(s if d == comp else s + 1 for d, s in enumerate(sizes))


def slab_shape(key, sizes):
    return tuple(s + 1 for k, s in zip(key, sizes) if not k)


def apply_kernel(counts, groups, nbufs, *refs):
    vec_ref, x_ref, y_ref, z_ref, xy_ref, xz_ref, yz_ref, hi_ref, lo_ref = refs[:9]
    res = refs[9:12]
    msgs = refs[12 : 12 + nbufs]
    ext_ref, elem_ref, out_ref, acc_ref = refs[12 + nbufs :]
    sizes = tuple(ORDER * c for c in counts)
    sx, sy, sz = sizes
    vecs = vec_ref.shape[-1]
    stride = acc_ref.shape[0] // (3 * (sx + 1) * (sy + 1))

    def at(comp, x, y):
        return 8 + ((comp * (sx + 1) + x) * (sy + 1) + y) * stride

    blank = jnp.zeros((8, vecs), F32)
    for comp in range(3):
        for x in range(sx + (comp != 0)):
            for y in range(sy + (comp != 1)):
                base = at(comp, x, y)
                for t in range(0, stride, 8):
                    if t + 8 > sz:
                        ext_ref[base + t : base + t + 8] = blank
                if x < sx and y < sy:
                    col = vec_ref[comp, x, y]
                elif x == sx and y == sy:
                    col = xy_ref[...]
                elif x == sx:
                    col = x_ref[comp - 1, y]
                else:
                    col = y_ref[0 if comp == 0 else 1, x]
                ext_ref[base : base + sz] = col
                if comp != 2:
                    if x == sx:
                        top = xz_ref[y : y + 1]
                    elif y == sy:
                        top = yz_ref[x : x + 1]
                    else:
                        top = z_ref[comp, x, y : y + 1]
                    ext_ref[base + sz : base + sz + 1] = top

    sub = lax.broadcasted_iota(jnp.int32, (8, vecs), 0)
    for i in range(counts[0]):
        for j in range(counts[1]):
            for k in range(counts[2]):
                e = (i * counts[1] + j) * counts[2] + k
                for comp in range(3):
                    shape = rows_of(comp)
                    columns = [(a, b) for a in range(shape[0]) for b in range(shape[1])]
                    for n in range(0, len(columns), 2):
                        (a, b), (a2, b2) = columns[n], columns[n + 1]
                        low = at(comp, 3 * i + a, 3 * j + b) + 3 * k
                        high = at(comp, 3 * i + a2, 3 * j + b2) + 3 * k - 4
                        tile = jnp.where(sub < 4, ext_ref[low : low + 8], ext_ref[high : high + 8])
                        row = STARTS[comp] + 4 * n
                        elem_ref[row : row + 8] = tile
                hi, lo = split(elem_ref[...])
                both = dot(hi_ref[e], jnp.concatenate([hi, lo], axis=1))
                out_ref[e, 8 : 8 + PADDED] = both[:, :vecs] + both[:, vecs:] + dot(lo_ref[e], hi)

    for comp in range(3):
        shape = rows_of(comp)
        for x in range(sx + (comp != 0)):
            for y in range(sy + (comp != 1)):
                for t in range(0, stride, 8):
                    total = None
                    for i in range(counts[0]):
                        a = x - 3 * i
                        if not 0 <= a < shape[0]:
                            continue
                        for j in range(counts[1]):
                            b = y - 3 * j
                            if not 0 <= b < shape[1]:
                                continue
                            row = 8 + STARTS[comp] + (a * shape[1] + b) * 4
                            for k in range(counts[2]):
                                first = 3 * k - t
                                if first >= 8 or first + shape[2] <= 0:
                                    continue
                                e = (i * counts[1] + j) * counts[2] + k
                                part = out_ref[e, row - first : row - first + 8]
                                keep = (sub >= first) & (sub < first + shape[2])
                                part = jnp.where(keep, part, 0.0)
                                total = part if total is None else total + part
                    if total is not None:
                        base = at(comp, x, y) - 8 + t
                        acc_ref[base : base + 8] = total

    length = [sz + 1, sz + 1, sz]
    for comp in range(3):
        for x in range(sx + (comp != 0)):
            for y in range(sy + (comp != 1)):
                base = at(comp, x, y) - 8
                res[comp][x, y] = acc_ref[base : base + length[comp]]

    for buf, keys in zip(msgs, groups):
        slot = 0
        for key in keys:
            for comp in plane_items(key):
                xs = range(sx + (comp != 0)) if not key[0] else [0 if key[0] < 0 else sx]
                ys = range(sy + (comp != 1)) if not key[1] else [0 if key[1] < 0 else sy]
                if key[2]:
                    z = 0 if key[2] < 0 else sz
                    if key[0]:
                        for y in ys:
                            base = at(comp, xs[0], y) - 8 + z
                            buf[slot, 0, y : y + 1] = acc_ref[base : base + 1]
                    elif key[1]:
                        for x in xs:
                            base = at(comp, x, ys[0]) - 8 + z
                            buf[slot, 0, x : x + 1] = acc_ref[base : base + 1]
                    else:
                        for x in xs:
                            for y in ys:
                                base = at(comp, x, y) - 8 + z
                                buf[slot, x, y : y + 1] = acc_ref[base : base + 1]
                else:
                    for n, (x, y) in enumerate((x, y) for x in xs for y in ys):
                        base = at(comp, x, y) - 8
                        buf[slot, n, : length[comp]] = acc_ref[base : base + length[comp]]
                slot += 1


def finish_kernel(counts, groups, nbufs, *refs):
    res = refs[:3]
    msgs = refs[3 : 3 + nbufs]
    outs = refs[3 + nbufs :]
    sizes = tuple(ORDER * c for c in counts)
    sx, sy, sz = sizes
    length = [sz + 1, sz + 1, sz]
    for comp in range(3):
        outs[comp][...] = res[comp][...]
    for buf, keys in zip(msgs, groups):
        slot = 0
        for key in keys:
            for comp in plane_items(key):
                xs = range(sx + (comp != 0)) if not key[0] else [sx if key[0] < 0 else 0]
                ys = range(sy + (comp != 1)) if not key[1] else [sy if key[1] < 0 else 0]
                out = outs[comp]
                if key[2]:
                    z = sz if key[2] < 0 else 0
                    if key[0]:
                        for y in ys:
                            out[xs[0], y, z : z + 1] += buf[slot, 0, y : y + 1]
                    elif key[1]:
                        for x in xs:
                            out[x, ys[0], z : z + 1] += buf[slot, 0, x : x + 1]
                    else:
                        for x in xs:
                            for y in ys:
                                out[x, y, z : z + 1] += buf[slot, x, y : y + 1]
                else:
                    for n, (x, y) in enumerate((x, y) for x in xs for y in ys):
                        out[x, y] += buf[slot, n, : length[comp]]
                slot += 1


def shift(array, offset, dims):
    used = [d for d in range(3) if offset[d] % dims[d]]
    names = tuple(AXES[d] for d in used)
    lens = [dims[d] for d in used]
    pairs = []
    for src in np.ndindex(*lens):
        dst = tuple((s + offset[d]) % dims[d] for s, d in zip(src, used))
        pairs.append((int(np.ravel_multi_index(src, lens)), int(np.ravel_multi_index(dst, lens))))
    return lax.ppermute(array, names, pairs)


def on_device(dims, vectors, orient_flip, reluctivity, conductivity):
    counts = (orient_flip.shape[0], orient_flip.shape[1], orient_flip.shape[2] // ELEM_DOFS)
    elements = counts[0] * counts[1] * counts[2]
    sx, sy, sz = vectors.shape[1:4]
    sizes = (sx, sy, sz)
    vecs = vectors.shape[4]
    params = pltpu.CompilerParams(vmem_limit_bytes=16 * 2**20)

    def shape(*dims_now, dtype=F32):
        return jax.ShapeDtypeStruct(dims_now, dtype)

    faces = pl.pallas_call(
        pack_kernel,
        out_shape=[
            shape(2, sy, sz, vecs),
            shape(2, sx, sz, vecs),
            shape(2, sx, sy, vecs),
            shape(sz, vecs),
            shape(sy, vecs),
            shape(sx, vecs),
        ],
        compiler_params=params,
        name="pack",
    )(vectors)
    offsets = [(-1, 0, 0), (0, -1, 0), (0, 0, -1), (-1, -1, 0), (-1, 0, -1), (0, -1, -1)]
    halo = [shift(face, offset, dims) for face, offset in zip(faces, offsets)]

    table, weight, place = element_tables()
    right = jnp.asarray(table, F32)
    right_hi = right.astype(BF16)
    right_lo = (right - right_hi.astype(F32)).astype(BF16)
    right_all = jnp.concatenate([right_hi, right_lo, right_hi], axis=0)
    left = jnp.asarray((table * weight[:, None]).T, F32)
    placed = np.zeros((counts[2], ELEM_DOFS * counts[2], PADDED))
    for k in range(counts[2]):
        placed[k, ELEM_DOFS * k : ELEM_DOFS * (k + 1)] = place
    mat_hi, mat_lo = pl.pallas_call(
        functools.partial(form_kernel, counts),
        out_shape=[shape(elements, PADDED, PADDED, dtype=BF16)] * 2,
        compiler_params=params,
        cost_estimate=pl.CostEstimate(
            flops=elements * PADDED * PADDED * 384 * 6, bytes_accessed=2000000, transcendentals=0
        ),
        name="form",
    )(
        left,
        right_all,
        jnp.asarray(placed, BF16),
        jnp.asarray(placed.transpose(0, 2, 1), F32),
        orient_flip,
        reluctivity,
        conductivity,
    )

    grouped = message_groups(dims)
    groups = list(grouped.values())
    targets = list(grouped.keys())
    buffers = []
    for keys in groups:
        slots = sum(len(plane_items(key)) for key in keys)
        key = keys[0]
        free = [s for k, s in zip(key, sizes) if not k]
        buffers.append(shape(slots, free[0] + 1, free[1] + 1, vecs) if len(free) == 2 else shape(slots, 1, free[0], vecs))
    stride = -(-(sz + 1) // 8) * 8
    rows = 3 * (sx + 1) * (sy + 1) * stride
    results = [shape(*region_shape(c, sizes), vecs) for c in range(3)]
    parts = pl.pallas_call(
        functools.partial(apply_kernel, counts, groups, len(buffers)),
        out_shape=results + buffers,
        scratch_shapes=[
            pltpu.VMEM((rows + 16, vecs), F32),
            pltpu.VMEM((PADDED, vecs), F32),
            pltpu.VMEM((elements, PADDED + 16, vecs), F32),
            pltpu.VMEM((rows, vecs), F32),
        ],
        compiler_params=params,
        cost_estimate=pl.CostEstimate(
            flops=elements * PADDED * PADDED * vecs * 6, bytes_accessed=3000000, transcendentals=0
        ),
        name="apply",
    )(vectors, *halo, mat_hi, mat_lo)
    arrived = [shift(buf, target, dims) for buf, target in zip(parts[3:], targets)]
    return pl.pallas_call(
        functools.partial(finish_kernel, counts, groups, len(buffers)),
        out_shape=results,
        compiler_params=params,
        name="finish",
    )(*parts[:3], *arrived)


def solution(mesh):
    dims = tuple(mesh.shape[axis] for axis in AXES)
    spec = P("gx", "gy", "gz")
    out = P("gx", "gy", "gz", None)
    return jax.shard_map(
        functools.partial(on_device, dims),
        mesh=mesh,
        in_specs=(P(None, "gx", "gy", "gz", None), spec, spec, spec),
        out_specs=(out, out, out),
        check_vma=False,
    )
```

```python
import functools

import jax
import jax.numpy as jnp
import numpy as np
from jax import lax
from jax.experimental import pallas as pl
from jax.experimental.pallas import tpu as pltpu
from jax.sharding import PartitionSpec as P

ORDER = 3
QUAD = 4
ELEM_DOFS = 144
QPTS = 64
AXES = ("gx", "gy", "gz")
F32 = jnp.float32
BF16 = jnp.bfloat16


def lagrange(points_at, evaluate_at):
    amount = len(points_at)
    values = np.ones((len(evaluate_at), amount))
    slopes = np.zeros((len(evaluate_at), amount))
    for which in range(amount):
        for column in range(amount):
            if column != which:
                factor = (evaluate_at - points_at[column]) / (points_at[which] - points_at[column])
                slopes[:, which] = slopes[:, which] * factor + values[:, which] / (
                    points_at[which] - points_at[column]
                )
                values[:, which] = values[:, which] * factor
    return (values, slopes)


def rows_of(comp):
    shape = [ORDER + 1] * 3
    shape[comp] = ORDER
    return shape


STARTS = (0, 48, 96)
PADDED = 160


def element_tables():
    lobatto = np.array([0.0, (1 - 5 ** (-0.5)) / 2, (1 + 5 ** (-0.5)) / 2, 1.0])
    gauss_open = np.array([(1 - 0.6**0.5) / 2, 0.5, (1 + 0.6**0.5) / 2])
    inner_pt = (3.0 / 7 - 2.0 / 7 * (6.0 / 5) ** 0.5) ** 0.5
    outer_pt = (3.0 / 7 + 2.0 / 7 * (6.0 / 5) ** 0.5) ** 0.5
    inner_wt = (18 + 30**0.5) / 36
    outer_wt = (18 - 30**0.5) / 36
    quad_points = (1 + np.array([-outer_pt, -inner_pt, inner_pt, outer_pt])) / 2
    quad_weight = np.array([outer_wt, inner_wt, inner_wt, outer_wt]) / 2
    closed, slopes = lagrange(lobatto, quad_points)
    opened, _ = lagrange(gauss_open, quad_points)
    weight = np.einsum("i,j,k->ijk", quad_weight, quad_weight, quad_weight).reshape(-1)

    def table(comp, deriv=None):
        mats = [opened if d == comp else (slopes if d == deriv else closed) for d in range(3)]
        return np.einsum("qa,rb,sc->qrsabc", *mats).reshape(QPTS, -1)

    full = np.zeros((6, QPTS, 3, 48))
    for comp in range(3):
        full[comp, :, comp] = table(comp)
    for out in range(3):
        first, second = (out + 1) % 3, (out + 2) % 3
        full[3 + out, :, second] += table(second, first)
        full[3 + out, :, first] -= table(first, second)
    full = full.reshape(6 * QPTS, ELEM_DOFS)
    place = np.zeros((ELEM_DOFS, PADDED))
    for comp in range(3):
        shape = rows_of(comp)
        for d in range(48):
            a, b, c = np.unravel_index(d, shape)
            place[48 * comp + d, STARTS[comp] + (a * shape[1] + b) * 4 + c] = 1
    return full @ place, np.tile(weight, 6), place


def split(x):
    hi = x.astype(BF16)
    return hi, (x - hi.astype(F32)).astype(BF16)


def dot(a, b):
    return jnp.dot(a, b, preferred_element_type=F32)


def dot_t(a, b):
    return lax.dot_general(a, b, (((1,), (1,)), ((), ())), preferred_element_type=F32)


def form_kernel(counts, wt_ref, place_ref, flip_ref, rel_ref, con_ref, hi_ref, lo_ref):
    count_x, count_y, count_z = counts
    lanes = ELEM_DOFS * count_z
    table = wt_ref[:PADDED]
    weight = wt_ref[PADDED : PADDED + 1]
    hi, lo = split(table)
    right = jnp.concatenate([hi, lo, hi], axis=1)
    for i in range(count_x):
        for j in range(count_y):
            sign = 1.0 - 2.0 * flip_ref[i, j : j + 1, :].astype(F32)
            signs = jnp.broadcast_to(sign, (PADDED, lanes)).astype(BF16)
            con_all = con_ref[i, j : j + 1, :]
            rel_all = rel_ref[i, j : j + 1, :]
            for k in range(count_z):
                e = (i * count_y + j) * count_z + k
                con = con_all[:, QPTS * k : QPTS * (k + 1)]
                rel = rel_all[:, QPTS * k : QPTS * (k + 1)]
                scale = jnp.concatenate([con, con, con, rel, rel, rel], axis=1) * weight
                hi, lo = split(table * scale)
                mat = dot_t(jnp.concatenate([hi, hi, lo], axis=1), right)
                row = dot_t(signs[:16], place_ref[k])[0:1]
                col = dot_t(place_ref[k], signs)
                hi, lo = split(mat * row * col)
                hi_ref[e] = hi
                lo_ref[e] = lo


def pack_kernel(src_ref, wt_src, place_src, *refs):
    x_ref, y_ref, z_ref, xy_ref, xz_ref, yz_ref, vec_ref, wt_ref, place_ref, sems = refs
    copies = [
        pltpu.make_async_copy(src, dst, sems.at[n])
        for n, (src, dst) in enumerate(
            ((src_ref, vec_ref), (wt_src, wt_ref), (place_src, place_ref))
        )
    ]
    for copy in copies:
        copy.start()
    copies[0].wait()
    x_ref[0] = vec_ref[1, 0]
    x_ref[1] = vec_ref[2, 0]
    y_ref[0] = vec_ref[0, :, 0]
    y_ref[1] = vec_ref[2, :, 0]
    z_ref[0] = vec_ref[0, :, :, 0]
    z_ref[1] = vec_ref[1, :, :, 0]
    xy_ref[...] = vec_ref[2, 0, 0]
    xz_ref[...] = vec_ref[1, 0, :, 0]
    yz_ref[...] = vec_ref[0, :, 0, 0]
    for copy in copies[1:]:
        copy.wait()


def face_groups(axis, dims):
    groups = {}
    for up in (-1, 1):
        groups.setdefault(up % dims[axis], []).append(up)
    return groups


def region_shape(comp, sizes):
    return tuple(s if d == comp else s + 1 for d, s in enumerate(sizes))


def face_shape(axis, keys, sizes, vecs):
    first, second = (s + 1 for d, s in enumerate(sizes) if d != axis)
    return jax.ShapeDtypeStruct((2 * len(keys), first, second, vecs), F32)


def face_rows(axis, keys, sizes, sent):
    slot = 0
    for up in keys:
        low = (up < 0) == sent
        for comp in (c for c in range(3) if c != axis):
            shape = region_shape(comp, sizes)
            edge = 0 if low else sizes[axis]
            if axis == 0:
                yield from ((slot, comp, (y,), edge, y, slice(0, shape[2])) for y in range(shape[1]))
            elif axis == 1:
                yield from ((slot, comp, (x,), x, edge, slice(0, shape[2])) for x in range(shape[0]))
            else:
                for x in range(shape[0]):
                    for y in range(shape[1]):
                        yield (slot, comp, (x, slice(y, y + 1)), x, y, slice(edge, edge + 1))
            slot += 1


def put_faces(axis, groups, sizes, res, bufs):
    for buf, keys in zip(bufs, groups):
        for slot, comp, place, x, y, z in face_rows(axis, keys, sizes, True):
            if axis == 2:
                buf[(slot,) + place] = res[comp][x, y, z]
            else:
                buf[slot, place[0], z] = res[comp][x, y, z]


def add_faces(axis, groups, sizes, res, bufs):
    for buf, keys in zip(bufs, groups):
        for slot, comp, place, x, y, z in face_rows(axis, keys, sizes, False):
            if axis == 2:
                res[comp][x, y, z] += buf[(slot,) + place]
            else:
                res[comp][x, y, z] += buf[slot, place[0], z]


def middle_kernel(axis, groups_in, groups_out, sizes, *refs):
    n_in = len(groups_in)
    old, bufs, res, out = refs[:3], refs[3 : 3 + n_in], refs[3 + n_in : 6 + n_in], refs[6 + n_in :]
    for comp in range(3):
        res[comp][...] = old[comp][...]
    add_faces(axis, groups_in, sizes, res, bufs)
    put_faces(axis + 1, groups_out, sizes, res, out)


def last_kernel(axis, groups, sizes, *refs):
    count = len(groups)
    old, bufs, res = refs[:3], refs[3 : 3 + count], refs[3 + count :]
    for comp in range(2):
        res[comp][...] = old[comp][...]
    for x in range(old[2].shape[0]):
        for y in range(old[2].shape[1]):
            res[2][x, :, y] = old[2][x, y]
    add_faces(axis, groups, sizes, res, bufs)


def apply_kernel(counts, groups, *refs):
    vec_ref, x_ref, y_ref, z_ref, xy_ref, xz_ref, yz_ref, hi_ref, lo_ref = refs[:9]
    res = refs[9:12]
    msgs = refs[12 : 12 + len(groups)]
    ext_ref, elem_ref, out_ref, acc_ref = refs[12 + len(groups) :]
    sizes = tuple(ORDER * c for c in counts)
    sx, sy, sz = sizes
    vecs = vec_ref.shape[-1]
    stride = acc_ref.shape[0] // (3 * (sx + 1) * (sy + 1))

    def at(comp, x, y):
        return 8 + ((comp * (sx + 1) + x) * (sy + 1) + y) * stride

    blank = jnp.zeros((8, vecs), F32)
    for comp in range(3):
        for x in range(sx + (comp != 0)):
            for y in range(sy + (comp != 1)):
                base = at(comp, x, y)
                for t in range(0, stride, 8):
                    if t + 8 > sz:
                        ext_ref[base + t : base + t + 8] = blank
                if x < sx and y < sy:
                    col = vec_ref[comp, x, y]
                elif x == sx and y == sy:
                    col = xy_ref[...]
                elif x == sx:
                    col = x_ref[comp - 1, y]
                else:
                    col = y_ref[0 if comp == 0 else 1, x]
                ext_ref[base : base + sz] = col
                if comp != 2:
                    if x == sx:
                        top = xz_ref[y : y + 1]
                    elif y == sy:
                        top = yz_ref[x : x + 1]
                    else:
                        top = z_ref[comp, x, y : y + 1]
                    ext_ref[base + sz : base + sz + 1] = top

    sub = lax.broadcasted_iota(jnp.int32, (8, vecs), 0)
    for i in range(counts[0]):
        for j in range(counts[1]):
            for k in range(counts[2]):
                e = (i * counts[1] + j) * counts[2] + k
                for comp in range(3):
                    shape = rows_of(comp)
                    columns = [(a, b) for a in range(shape[0]) for b in range(shape[1])]
                    for n in range(0, len(columns), 2):
                        (a, b), (a2, b2) = columns[n], columns[n + 1]
                        low = at(comp, 3 * i + a, 3 * j + b) + 3 * k
                        high = at(comp, 3 * i + a2, 3 * j + b2) + 3 * k - 4
                        tile = jnp.where(sub < 4, ext_ref[low : low + 8], ext_ref[high : high + 8])
                        row = STARTS[comp] + 4 * n
                        elem_ref[row : row + 8] = tile
                hi, lo = split(elem_ref[...])
                both = dot(hi_ref[e], jnp.concatenate([hi, lo], axis=1))
                out_ref[e, 8 : 8 + PADDED] = both[:, :vecs] + both[:, vecs:] + dot(lo_ref[e], hi)

    for comp in range(3):
        shape = rows_of(comp)
        for x in range(sx + (comp != 0)):
            for y in range(sy + (comp != 1)):
                for t in range(0, stride, 8):
                    total = None
                    for i in range(counts[0]):
                        a = x - 3 * i
                        if not 0 <= a < shape[0]:
                            continue
                        for j in range(counts[1]):
                            b = y - 3 * j
                            if not 0 <= b < shape[1]:
                                continue
                            row = 8 + STARTS[comp] + (a * shape[1] + b) * 4
                            for k in range(counts[2]):
                                first = 3 * k - t
                                if first >= 8 or first + shape[2] <= 0:
                                    continue
                                e = (i * counts[1] + j) * counts[2] + k
                                part = out_ref[e, row - first : row - first + 8]
                                keep = (sub >= first) & (sub < first + shape[2])
                                part = jnp.where(keep, part, 0.0)
                                total = part if total is None else total + part
                    if total is not None:
                        base = at(comp, x, y) - 8 + t
                        acc_ref[base : base + 8] = total

    length = [sz + 1, sz + 1, sz]
    for comp in range(3):
        for x in range(sx + (comp != 0)):
            for y in range(sy + (comp != 1)):
                base = at(comp, x, y) - 8
                res[comp][x, y] = acc_ref[base : base + length[comp]]

    put_faces(0, groups, sizes, res, msgs)


def shift(array, offset, dims):
    used = [d for d in range(3) if offset[d] % dims[d]]
    names = tuple(AXES[d] for d in used)
    lens = [dims[d] for d in used]
    pairs = []
    for src in np.ndindex(*lens):
        dst = tuple((s + offset[d]) % dims[d] for s, d in zip(src, used))
        pairs.append((int(np.ravel_multi_index(src, lens)), int(np.ravel_multi_index(dst, lens))))
    return lax.ppermute(array, names, pairs)


def on_device(dims, vectors, orient_flip, reluctivity, conductivity):
    counts = (orient_flip.shape[0], orient_flip.shape[1], orient_flip.shape[2] // ELEM_DOFS)
    elements = counts[0] * counts[1] * counts[2]
    sx, sy, sz = vectors.shape[1:4]
    sizes = (sx, sy, sz)
    vecs = vectors.shape[4]
    params = pltpu.CompilerParams(vmem_limit_bytes=16 * 2**20)

    def shape(*dims_now, dtype=F32):
        return jax.ShapeDtypeStruct(dims_now, dtype)

    table, weight, place = element_tables()
    scaled = np.zeros((PADDED + 8, 6 * QPTS))
    scaled[:PADDED] = table.T
    scaled[PADDED] = weight
    placed = np.zeros((counts[2], PADDED, ELEM_DOFS * counts[2]))
    for k in range(counts[2]):
        placed[k, :, ELEM_DOFS * k : ELEM_DOFS * (k + 1)] = place.T
    scaled = jnp.asarray(scaled, F32)
    placed = jnp.asarray(placed, BF16)
    *faces, held, scaled, placed = pl.pallas_call(
        pack_kernel,
        in_specs=[pl.BlockSpec(memory_space=pltpu.MemorySpace.HBM)] * 3,
        out_shape=[
            shape(2, sy, sz, vecs),
            shape(2, sx, sz, vecs),
            shape(2, sx, sy, vecs),
            shape(sz, vecs),
            shape(sy, vecs),
            shape(sx, vecs),
            shape(*vectors.shape),
            shape(*scaled.shape),
            shape(*placed.shape, dtype=BF16),
        ],
        scratch_shapes=[pltpu.SemaphoreType.DMA((3,))],
        compiler_params=params,
        name="pack",
    )(vectors, scaled, placed)
    offsets = [(-1, 0, 0), (0, -1, 0), (0, 0, -1), (-1, -1, 0), (-1, 0, -1), (0, -1, -1)]
    halo = [shift(face, offset, dims) for face, offset in zip(faces, offsets)]
    mat_hi, mat_lo = pl.pallas_call(
        functools.partial(form_kernel, counts),
        out_shape=[shape(elements, PADDED, PADDED, dtype=BF16)] * 2,
        compiler_params=params,
        cost_estimate=pl.CostEstimate(
            flops=elements * PADDED * PADDED * 384 * 6, bytes_accessed=2000000, transcendentals=0
        ),
        name="form",
    )(scaled, placed, orient_flip, reluctivity, conductivity)

    grouped = [face_groups(axis, dims) for axis in range(3)]
    groups = [list(g.values()) for g in grouped]
    buffers = [[face_shape(axis, keys, sizes, vecs) for keys in groups[axis]] for axis in range(3)]
    stride = -(-(sz + 1) // 8) * 8
    rows = 3 * (sx + 1) * (sy + 1) * stride
    results = [shape(*region_shape(c, sizes), vecs) for c in range(3)]

    def send(axis, bufs):
        return [
            shift(buf, [by if d == axis else 0 for d in range(3)], dims)
            for buf, by in zip(bufs, grouped[axis])
        ]

    parts = pl.pallas_call(
        functools.partial(apply_kernel, counts, groups[0]),
        out_shape=results + buffers[0],
        scratch_shapes=[
            pltpu.VMEM((rows + 16, vecs), F32),
            pltpu.VMEM((PADDED, vecs), F32),
            pltpu.VMEM((elements, PADDED + 16, vecs), F32),
            pltpu.VMEM((rows, vecs), F32),
        ],
        compiler_params=params,
        cost_estimate=pl.CostEstimate(
            flops=elements * PADDED * PADDED * vecs * 6, bytes_accessed=3000000, transcendentals=0
        ),
        name="apply",
    )(held, *halo, mat_hi, mat_lo)
    for axis in range(2):
        parts = pl.pallas_call(
            functools.partial(middle_kernel, axis, groups[axis], groups[axis + 1], sizes),
            out_shape=results + buffers[axis + 1],
            compiler_params=params,
            name=f"middle_{axis}",
        )(*parts[:3], *send(axis, parts[3:]))
    out_z = shape(sx + 1, sz, sy + 1, vecs)
    outs = pl.pallas_call(
        functools.partial(last_kernel, 2, groups[2], sizes),
        out_shape=results[:2] + [out_z],
        compiler_params=params,
        name="last",
    )(*parts[:3], *send(2, parts[3:]))
    return outs[0], outs[1], jnp.swapaxes(outs[2], 1, 2)


def solution(mesh):
    dims = tuple(mesh.shape[axis] for axis in AXES)
    spec = P("gx", "gy", "gz")
    out = P("gx", "gy", "gz", None)
    return jax.shard_map(
        functools.partial(on_device, dims),
        mesh=mesh,
        in_specs=(P(None, "gx", "gy", "gz", None), spec, spec, spec),
        out_specs=(out, out, out),
        check_vma=False,
    )
```

```python
import functools

import jax
import jax.numpy as jnp
import numpy as np
from jax import lax
from jax.experimental import pallas as pl
from jax.experimental.pallas import tpu as pltpu
from jax.sharding import PartitionSpec as P

ORDER = 3
QUAD = 4
ELEM_DOFS = 144
QPTS = 64
AXES = ("gx", "gy", "gz")
F32 = jnp.float32
BF16 = jnp.bfloat16


def lagrange(points_at, evaluate_at):
    amount = len(points_at)
    values = np.ones((len(evaluate_at), amount))
    slopes = np.zeros((len(evaluate_at), amount))
    for which in range(amount):
        for column in range(amount):
            if column != which:
                factor = (evaluate_at - points_at[column]) / (points_at[which] - points_at[column])
                slopes[:, which] = slopes[:, which] * factor + values[:, which] / (
                    points_at[which] - points_at[column]
                )
                values[:, which] = values[:, which] * factor
    return (values, slopes)


def rows_of(comp):
    shape = [ORDER + 1] * 3
    shape[comp] = ORDER
    return shape


STARTS = (0, 48, 96)
PADDED = 160


def element_tables():
    lobatto = np.array([0.0, (1 - 5 ** (-0.5)) / 2, (1 + 5 ** (-0.5)) / 2, 1.0])
    gauss_open = np.array([(1 - 0.6**0.5) / 2, 0.5, (1 + 0.6**0.5) / 2])
    inner_pt = (3.0 / 7 - 2.0 / 7 * (6.0 / 5) ** 0.5) ** 0.5
    outer_pt = (3.0 / 7 + 2.0 / 7 * (6.0 / 5) ** 0.5) ** 0.5
    inner_wt = (18 + 30**0.5) / 36
    outer_wt = (18 - 30**0.5) / 36
    quad_points = (1 + np.array([-outer_pt, -inner_pt, inner_pt, outer_pt])) / 2
    quad_weight = np.array([outer_wt, inner_wt, inner_wt, outer_wt]) / 2
    closed, slopes = lagrange(lobatto, quad_points)
    opened, _ = lagrange(gauss_open, quad_points)
    weight = np.einsum("i,j,k->ijk", quad_weight, quad_weight, quad_weight).reshape(-1)

    def table(comp, deriv=None):
        mats = [opened if d == comp else (slopes if d == deriv else closed) for d in range(3)]
        return np.einsum("qa,rb,sc->qrsabc", *mats).reshape(QPTS, -1)

    full = np.zeros((6, QPTS, 3, 48))
    for comp in range(3):
        full[comp, :, comp] = table(comp)
    for out in range(3):
        first, second = (out + 1) % 3, (out + 2) % 3
        full[3 + out, :, second] += table(second, first)
        full[3 + out, :, first] -= table(first, second)
    full = full.reshape(6 * QPTS, ELEM_DOFS)
    place = np.zeros((ELEM_DOFS, PADDED))
    for comp in range(3):
        shape = rows_of(comp)
        for d in range(48):
            a, b, c = np.unravel_index(d, shape)
            place[48 * comp + d, STARTS[comp] + (a * shape[1] + b) * 4 + c] = 1
    return full @ place, np.tile(weight, 6), place


def split(x):
    hi = x.astype(BF16)
    return hi, (x - hi.astype(F32)).astype(BF16)


def dot(a, b):
    return jnp.dot(a, b, preferred_element_type=F32)


def dot_t(a, b):
    return lax.dot_general(a, b, (((1,), (1,)), ((), ())), preferred_element_type=F32)


def form_kernel(counts, const_ref, flip_ref, rel_ref, con_ref, hi_ref, lo_ref):
    count_x, count_y, count_z = counts
    lanes = ELEM_DOFS * count_z
    table = const_ref[:PADDED, : 6 * QPTS]
    weight = const_ref[PADDED : PADDED + 1, : 6 * QPTS]
    first = PADDED + 8
    places = [
        const_ref[first + PADDED * k : first + PADDED * (k + 1), :lanes].astype(BF16)
        for k in range(count_z)
    ]
    hi, lo = split(table)
    right = jnp.concatenate([hi, lo, hi], axis=1)
    for i in range(count_x):
        for j in range(count_y):
            sign = 1.0 - 2.0 * flip_ref[i, j : j + 1, :].astype(F32)
            signs = jnp.broadcast_to(sign, (PADDED, lanes)).astype(BF16)
            con_all = con_ref[i, j : j + 1, :]
            rel_all = rel_ref[i, j : j + 1, :]
            for k in range(count_z):
                e = (i * count_y + j) * count_z + k
                con = con_all[:, QPTS * k : QPTS * (k + 1)]
                rel = rel_all[:, QPTS * k : QPTS * (k + 1)]
                scale = jnp.concatenate([con, con, con, rel, rel, rel], axis=1) * weight
                hi, lo = split(table * scale)
                mat = dot_t(jnp.concatenate([hi, hi, lo], axis=1), right)
                row = dot_t(signs[:16], places[k])[0:1]
                col = dot_t(places[k], signs)
                hi, lo = split(mat * row * col)
                hi_ref[e] = hi
                lo_ref[e] = lo


def pack_kernel(vec_ref, x_ref, y_ref, z_ref, xy_ref, xz_ref, yz_ref):
    sx, sy, sz = vec_ref.shape[1:4]
    for slot, comp in enumerate((1, 2)):
        for y in range(sy):
            row = (slot * sy + y) * sz
            x_ref[row : row + sz] = vec_ref[comp, 0, y]
    for slot, comp in enumerate((0, 2)):
        for x in range(sx):
            row = (slot * sx + x) * sz
            y_ref[row : row + sz] = vec_ref[comp, x, 0]
    for comp in (0, 1):
        for x in range(sx):
            row = (comp * sx + x) * sy
            z_ref[row : row + sy] = vec_ref[comp, x, :, 0]
    xy_ref[...] = vec_ref[2, 0, 0]
    xz_ref[...] = vec_ref[1, 0, :, 0]
    yz_ref[...] = vec_ref[0, :, 0, 0]


def face_groups(axis, dims):
    groups = {}
    for up in (-1, 1):
        groups.setdefault(up % dims[axis], []).append(up)
    return groups


def region_shape(comp, sizes):
    return tuple(s if d == comp else s + 1 for d, s in enumerate(sizes))


def face_shape(axis, keys, sizes, vecs):
    total = sum(z.stop - z.start for _, _, _, _, z in face_rows(axis, keys, sizes, True))
    return jax.ShapeDtypeStruct((total, vecs), F32)


def face_rows(axis, keys, sizes, sent):
    row = 0
    for up in keys:
        low = (up < 0) == sent
        for comp in (c for c in range(3) if c != axis):
            shape = region_shape(comp, sizes)
            edge = 0 if low else sizes[axis]
            spans = [range(n) for n in shape]
            spans[axis] = [edge]
            z = slice(edge, edge + 1) if axis == 2 else slice(0, shape[2])
            for x in spans[0]:
                for y in spans[1]:
                    yield (row, comp, x, y, z)
                    row += z.stop - z.start


def put_faces(axis, groups, sizes, res, bufs):
    for buf, keys in zip(bufs, groups):
        for row, comp, x, y, z in face_rows(axis, keys, sizes, True):
            buf[row : row + z.stop - z.start] = res[comp][x, y, z]


def add_faces(axis, groups, sizes, res, bufs):
    for buf, keys in zip(bufs, groups):
        for row, comp, x, y, z in face_rows(axis, keys, sizes, False):
            res[comp][x, y, z] += buf[row : row + z.stop - z.start]


def middle_kernel(axis, groups_in, groups_out, sizes, *refs):
    n_in = len(groups_in)
    old, bufs, res, out = refs[:3], refs[3 : 3 + n_in], refs[3 + n_in : 6 + n_in], refs[6 + n_in :]
    for comp in range(3):
        res[comp][...] = old[comp][...]
    add_faces(axis, groups_in, sizes, res, bufs)
    put_faces(axis + 1, groups_out, sizes, res, out)


def last_kernel(axis, groups, sizes, *refs):
    count = len(groups)
    old, bufs, res = refs[:3], refs[3 : 3 + count], refs[3 + count :]
    for comp in range(2):
        res[comp][...] = old[comp][...]
    for x in range(old[2].shape[0]):
        for y in range(old[2].shape[1]):
            res[2][x, :, y] = old[2][x, y]
    add_faces(axis, groups, sizes, res, bufs)


def apply_kernel(counts, groups, *refs):
    vec_ref, x_ref, y_ref, z_ref, xy_ref, xz_ref, yz_ref, hi_ref, lo_ref = refs[:9]
    res = refs[9:12]
    msgs = refs[12 : 12 + len(groups)]
    ext_ref, elem_ref, out_ref, acc_ref = refs[12 + len(groups) :]
    sizes = tuple(ORDER * c for c in counts)
    sx, sy, sz = sizes
    vecs = vec_ref.shape[-1]
    stride = acc_ref.shape[0] // (3 * (sx + 1) * (sy + 1))

    def at(comp, x, y):
        return 8 + ((comp * (sx + 1) + x) * (sy + 1) + y) * stride

    blank = jnp.zeros((8, vecs), F32)
    for comp in range(3):
        for x in range(sx + (comp != 0)):
            for y in range(sy + (comp != 1)):
                base = at(comp, x, y)
                for t in range(0, stride, 8):
                    if t + 8 > sz:
                        ext_ref[base + t : base + t + 8] = blank
                if x < sx and y < sy:
                    col = vec_ref[comp, x, y]
                elif x == sx and y == sy:
                    col = xy_ref[...]
                elif x == sx:
                    row = ((comp - 1) * sy + y) * sz
                    col = x_ref[row : row + sz]
                else:
                    row = ((comp != 0) * sx + x) * sz
                    col = y_ref[row : row + sz]
                ext_ref[base : base + sz] = col
                if comp != 2:
                    if x == sx:
                        top = xz_ref[y : y + 1]
                    elif y == sy:
                        top = yz_ref[x : x + 1]
                    else:
                        row = (comp * sx + x) * sy + y
                        top = z_ref[row : row + 1]
                    ext_ref[base + sz : base + sz + 1] = top

    sub = lax.broadcasted_iota(jnp.int32, (8, vecs), 0)
    for i in range(counts[0]):
        for j in range(counts[1]):
            for k in range(counts[2]):
                e = (i * counts[1] + j) * counts[2] + k
                for comp in range(3):
                    shape = rows_of(comp)
                    columns = [(a, b) for a in range(shape[0]) for b in range(shape[1])]
                    for n in range(0, len(columns), 2):
                        (a, b), (a2, b2) = columns[n], columns[n + 1]
                        low = at(comp, 3 * i + a, 3 * j + b) + 3 * k
                        high = at(comp, 3 * i + a2, 3 * j + b2) + 3 * k - 4
                        tile = jnp.where(sub < 4, ext_ref[low : low + 8], ext_ref[high : high + 8])
                        row = STARTS[comp] + 4 * n
                        elem_ref[row : row + 8] = tile
                hi, lo = split(elem_ref[...])
                both = dot(hi_ref[e], jnp.concatenate([hi, lo], axis=1))
                out_ref[e, 8 : 8 + PADDED] = both[:, :vecs] + both[:, vecs:] + dot(lo_ref[e], hi)

    for comp in range(3):
        shape = rows_of(comp)
        for x in range(sx + (comp != 0)):
            for y in range(sy + (comp != 1)):
                for t in range(0, stride, 8):
                    total = None
                    for i in range(counts[0]):
                        a = x - 3 * i
                        if not 0 <= a < shape[0]:
                            continue
                        for j in range(counts[1]):
                            b = y - 3 * j
                            if not 0 <= b < shape[1]:
                                continue
                            row = 8 + STARTS[comp] + (a * shape[1] + b) * 4
                            for k in range(counts[2]):
                                first = 3 * k - t
                                if first >= 8 or first + shape[2] <= 0:
                                    continue
                                e = (i * counts[1] + j) * counts[2] + k
                                part = out_ref[e, row - first : row - first + 8]
                                keep = (sub >= first) & (sub < first + shape[2])
                                part = jnp.where(keep, part, 0.0)
                                total = part if total is None else total + part
                    if total is not None:
                        base = at(comp, x, y) - 8 + t
                        acc_ref[base : base + 8] = total

    length = [sz + 1, sz + 1, sz]
    for comp in range(3):
        for x in range(sx + (comp != 0)):
            for y in range(sy + (comp != 1)):
                base = at(comp, x, y) - 8
                res[comp][x, y] = acc_ref[base : base + length[comp]]

    put_faces(0, groups, sizes, res, msgs)


def shift(array, offset, dims):
    used = [d for d in range(3) if offset[d] % dims[d]]
    names = tuple(AXES[d] for d in used)
    lens = [dims[d] for d in used]
    pairs = []
    for src in np.ndindex(*lens):
        dst = tuple((s + offset[d]) % dims[d] for s, d in zip(src, used))
        pairs.append((int(np.ravel_multi_index(src, lens)), int(np.ravel_multi_index(dst, lens))))
    return lax.ppermute(array, names, pairs)


def on_device(dims, vectors, orient_flip, reluctivity, conductivity):
    counts = (orient_flip.shape[0], orient_flip.shape[1], orient_flip.shape[2] // ELEM_DOFS)
    elements = counts[0] * counts[1] * counts[2]
    sx, sy, sz = vectors.shape[1:4]
    sizes = (sx, sy, sz)
    vecs = vectors.shape[4]
    params = pltpu.CompilerParams(vmem_limit_bytes=16 * 2**20)

    def shape(*dims_now, dtype=F32):
        return jax.ShapeDtypeStruct(dims_now, dtype)

    table, weight, place = element_tables()
    first = PADDED + 8
    lanes = ELEM_DOFS * counts[2]
    width = max(6 * QPTS, -(-lanes // 128) * 128)
    const = np.zeros((first + PADDED * counts[2], width))
    const[:PADDED, : 6 * QPTS] = table.T
    const[PADDED, : 6 * QPTS] = weight
    for k in range(counts[2]):
        rows = slice(first + PADDED * k, first + PADDED * (k + 1))
        const[rows, ELEM_DOFS * k : ELEM_DOFS * (k + 1)] = place.T
    faces = pl.pallas_call(
        pack_kernel,
        out_shape=[
            shape(2 * sy * sz, vecs),
            shape(2 * sx * sz, vecs),
            shape(2 * sx * sy, vecs),
            shape(sz, vecs),
            shape(sy, vecs),
            shape(sx, vecs),
        ],
        compiler_params=params,
        name="pack",
    )(vectors)
    offsets = [(-1, 0, 0), (0, -1, 0), (0, 0, -1), (-1, -1, 0), (-1, 0, -1), (0, -1, -1)]
    halo = [shift(face, offset, dims) for face, offset in zip(faces, offsets)]
    mat_hi, mat_lo = pl.pallas_call(
        functools.partial(form_kernel, counts),
        out_shape=[shape(elements, PADDED, PADDED, dtype=BF16)] * 2,
        compiler_params=params,
        cost_estimate=pl.CostEstimate(
            flops=elements * PADDED * PADDED * 384 * 6, bytes_accessed=2000000, transcendentals=0
        ),
        name="form",
    )(jnp.asarray(const, F32), orient_flip, reluctivity, conductivity)

    grouped = [face_groups(axis, dims) for axis in range(3)]
    groups = [list(g.values()) for g in grouped]
    buffers = [[face_shape(axis, keys, sizes, vecs) for keys in groups[axis]] for axis in range(3)]
    stride = -(-(sz + 1) // 8) * 8
    rows = 3 * (sx + 1) * (sy + 1) * stride
    results = [shape(*region_shape(c, sizes), vecs) for c in range(3)]

    def send(axis, bufs):
        return [
            shift(buf, [by if d == axis else 0 for d in range(3)], dims)
            for buf, by in zip(bufs, grouped[axis])
        ]

    parts = pl.pallas_call(
        functools.partial(apply_kernel, counts, groups[0]),
        out_shape=results + buffers[0],
        scratch_shapes=[
            pltpu.VMEM((rows + 16, vecs), F32),
            pltpu.VMEM((PADDED, vecs), F32),
            pltpu.VMEM((elements, PADDED + 16, vecs), F32),
            pltpu.VMEM((rows, vecs), F32),
        ],
        compiler_params=params,
        cost_estimate=pl.CostEstimate(
            flops=elements * PADDED * PADDED * vecs * 6, bytes_accessed=3000000, transcendentals=0
        ),
        name="apply",
    )(vectors, *halo, mat_hi, mat_lo)
    for axis in range(2):
        parts = pl.pallas_call(
            functools.partial(middle_kernel, axis, groups[axis], groups[axis + 1], sizes),
            out_shape=results + buffers[axis + 1],
            compiler_params=params,
            name=f"middle_{axis}",
        )(*parts[:3], *send(axis, parts[3:]))
    out_z = shape(sx + 1, sz, sy + 1, vecs)
    outs = pl.pallas_call(
        functools.partial(last_kernel, 2, groups[2], sizes),
        out_shape=results[:2] + [out_z],
        compiler_params=params,
        name="last",
    )(*parts[:3], *send(2, parts[3:]))
    return outs[0], outs[1], jnp.swapaxes(outs[2], 1, 2)


def solution(mesh):
    dims = tuple(mesh.shape[axis] for axis in AXES)
    spec = P("gx", "gy", "gz")
    out = P("gx", "gy", "gz", None)
    return jax.shard_map(
        functools.partial(on_device, dims),
        mesh=mesh,
        in_specs=(P(None, "gx", "gy", "gz", None), spec, spec, spec),
        out_specs=(out, out, out),
        check_vma=False,
    )
```

```python
import functools

import jax
import jax.numpy as jnp
import numpy as np
from jax import lax
from jax.experimental import pallas as pl
from jax.experimental.pallas import tpu as pltpu
from jax.sharding import PartitionSpec as P

ORDER = 3
QUAD = 4
ELEM_DOFS = 144
QPTS = 64
AXES = ("gx", "gy", "gz")
F32 = jnp.float32
BF16 = jnp.bfloat16


def lagrange(points_at, evaluate_at):
    amount = len(points_at)
    values = np.ones((len(evaluate_at), amount))
    slopes = np.zeros((len(evaluate_at), amount))
    for which in range(amount):
        for column in range(amount):
            if column != which:
                factor = (evaluate_at - points_at[column]) / (points_at[which] - points_at[column])
                slopes[:, which] = slopes[:, which] * factor + values[:, which] / (
                    points_at[which] - points_at[column]
                )
                values[:, which] = values[:, which] * factor
    return (values, slopes)


def rows_of(comp):
    shape = [ORDER + 1] * 3
    shape[comp] = ORDER
    return shape


STARTS = (0, 48, 96)
PADDED = 160


def element_tables():
    lobatto = np.array([0.0, (1 - 5 ** (-0.5)) / 2, (1 + 5 ** (-0.5)) / 2, 1.0])
    gauss_open = np.array([(1 - 0.6**0.5) / 2, 0.5, (1 + 0.6**0.5) / 2])
    inner_pt = (3.0 / 7 - 2.0 / 7 * (6.0 / 5) ** 0.5) ** 0.5
    outer_pt = (3.0 / 7 + 2.0 / 7 * (6.0 / 5) ** 0.5) ** 0.5
    inner_wt = (18 + 30**0.5) / 36
    outer_wt = (18 - 30**0.5) / 36
    quad_points = (1 + np.array([-outer_pt, -inner_pt, inner_pt, outer_pt])) / 2
    quad_weight = np.array([outer_wt, inner_wt, inner_wt, outer_wt]) / 2
    closed, slopes = lagrange(lobatto, quad_points)
    opened, _ = lagrange(gauss_open, quad_points)
    weight = np.einsum("i,j,k->ijk", quad_weight, quad_weight, quad_weight).reshape(-1)

    def table(comp, deriv=None):
        mats = [opened if d == comp else (slopes if d == deriv else closed) for d in range(3)]
        return np.einsum("qa,rb,sc->qrsabc", *mats).reshape(QPTS, -1)

    full = np.zeros((6, QPTS, 3, 48))
    for comp in range(3):
        full[comp, :, comp] = table(comp)
    for out in range(3):
        first, second = (out + 1) % 3, (out + 2) % 3
        full[3 + out, :, second] += table(second, first)
        full[3 + out, :, first] -= table(first, second)
    full = full.reshape(6 * QPTS, ELEM_DOFS)
    place = np.zeros((ELEM_DOFS, PADDED))
    for comp in range(3):
        shape = rows_of(comp)
        for d in range(48):
            a, b, c = np.unravel_index(d, shape)
            place[48 * comp + d, STARTS[comp] + (a * shape[1] + b) * 4 + c] = 1
    return full @ place, np.tile(weight, 6), place


def split(x):
    hi = x.astype(BF16)
    return hi, (x - hi.astype(F32)).astype(BF16)


def dot(a, b):
    return jnp.dot(a, b, preferred_element_type=F32)


def dot_t(a, b):
    return lax.dot_general(a, b, (((1,), (1,)), ((), ())), preferred_element_type=F32)


def form_kernel(counts, const_ref, flip_ref, rel_ref, con_ref, hi_ref, lo_ref):
    count_x, count_y, count_z = counts
    lanes = ELEM_DOFS * count_z
    table = const_ref[:PADDED, : 6 * QPTS]
    weight = const_ref[PADDED : PADDED + 1, : 6 * QPTS]
    first = PADDED + 8
    places = [
        const_ref[first + PADDED * k : first + PADDED * (k + 1), :lanes].astype(BF16)
        for k in range(count_z)
    ]
    hi, lo = split(table)
    right = jnp.concatenate([hi, lo, hi], axis=1)
    for i in range(count_x):
        for j in range(count_y):
            sign = 1.0 - 2.0 * flip_ref[i, j : j + 1, :].astype(F32)
            signs = jnp.broadcast_to(sign, (PADDED, lanes)).astype(BF16)
            con_all = con_ref[i, j : j + 1, :]
            rel_all = rel_ref[i, j : j + 1, :]
            for k in range(count_z):
                e = (i * count_y + j) * count_z + k
                con = con_all[:, QPTS * k : QPTS * (k + 1)]
                rel = rel_all[:, QPTS * k : QPTS * (k + 1)]
                scale = jnp.concatenate([con, con, con, rel, rel, rel], axis=1) * weight
                hi, lo = split(table * scale)
                mat = dot_t(jnp.concatenate([hi, hi, lo], axis=1), right)
                row = dot_t(signs[:16], places[k])[0:1]
                col = dot_t(places[k], signs)
                hi, lo = split(mat * row * col)
                hi_ref[e] = hi
                lo_ref[e] = lo


def pack_kernel(vec_ref, x_ref, y_ref, z_ref, xy_ref, xz_ref, yz_ref):
    sx, sy, sz = vec_ref.shape[1:4]
    for slot, comp in enumerate((1, 2)):
        for y in range(sy):
            row = (slot * sy + y) * sz
            x_ref[row : row + sz] = vec_ref[comp, 0, y]
    for slot, comp in enumerate((0, 2)):
        for x in range(sx):
            row = (slot * sx + x) * sz
            y_ref[row : row + sz] = vec_ref[comp, x, 0]
    for comp in (0, 1):
        for x in range(sx):
            row = (comp * sx + x) * sy
            z_ref[row : row + sy] = vec_ref[comp, x, :, 0]
    xy_ref[...] = vec_ref[2, 0, 0]
    xz_ref[...] = vec_ref[1, 0, :, 0]
    yz_ref[...] = vec_ref[0, :, 0, 0]


def face_groups(axis, dims):
    groups = {}
    if dims[axis] > 2 and dims[axis] % 2 == 0:
        return {"first": [0], "second": [2]}
    for up in (-1, 1):
        groups.setdefault(up % dims[axis], []).append(up)
    return groups


def region_shape(comp, sizes):
    return tuple(s if d == comp else s + 1 for d, s in enumerate(sizes))


def face_shape(axis, keys, sizes, vecs):
    total = sum(count for _, count, *_ in face_rows(axis, keys, sizes, True))
    return jax.ShapeDtypeStruct((total, vecs), F32)


def face_rows(axis, keys, sizes, sent):
    row = 0
    for up in keys:
        low = (up < 0) == sent
        for comp in (c for c in range(3) if c != axis):
            shape = region_shape(comp, sizes)
            edge = 0 if low else sizes[axis]
            if up in (0, 2):
                even = lax.rem(lax.axis_index(AXES[axis]) + up // 2, 2) == 0
                edge = jnp.where(even, sizes[axis], 0)
            spans = [range(n) for n in shape]
            spans[axis] = [edge]
            z = pl.ds(edge, 1) if axis == 2 else slice(0, shape[2])
            count = 1 if axis == 2 else shape[2]
            for x in spans[0]:
                for y in spans[1]:
                    yield (row, count, comp, x, y, z)
                    row += count


def put_faces(axis, groups, sizes, res, bufs):
    for buf, keys in zip(bufs, groups):
        for row, count, comp, x, y, z in face_rows(axis, keys, sizes, True):
            buf[row : row + count] = res[comp][x, y, z]


def add_faces(axis, groups, sizes, res, bufs):
    for buf, keys in zip(bufs, groups):
        for row, count, comp, x, y, z in face_rows(axis, keys, sizes, False):
            res[comp][x, y, z] += buf[row : row + count]


def middle_kernel(axis, groups_in, groups_out, sizes, *refs):
    n_in = len(groups_in)
    old, bufs, res, out = refs[:3], refs[3 : 3 + n_in], refs[3 + n_in : 6 + n_in], refs[6 + n_in :]
    for comp in range(3):
        res[comp][...] = old[comp][...]
    add_faces(axis, groups_in, sizes, res, bufs)
    put_faces(axis + 1, groups_out, sizes, res, out)


def last_kernel(axis, groups, sizes, *refs):
    count = len(groups)
    old, bufs, res = refs[:3], refs[3 : 3 + count], refs[3 + count :]
    for comp in range(2):
        res[comp][...] = old[comp][...]
    for x in range(old[2].shape[0]):
        for y in range(old[2].shape[1]):
            res[2][x, :, y] = old[2][x, y]
    add_faces(axis, groups, sizes, res, bufs)


def apply_kernel(counts, groups, *refs):
    vec_ref, x_ref, y_ref, z_ref, xy_ref, xz_ref, yz_ref, hi_ref, lo_ref = refs[:9]
    res = refs[9:12]
    msgs = refs[12 : 12 + len(groups)]
    ext_ref, elem_ref, out_ref, acc_ref = refs[12 + len(groups) :]
    sizes = tuple(ORDER * c for c in counts)
    sx, sy, sz = sizes
    vecs = vec_ref.shape[-1]
    stride = acc_ref.shape[0] // (3 * (sx + 1) * (sy + 1))

    def at(comp, x, y):
        return 8 + ((comp * (sx + 1) + x) * (sy + 1) + y) * stride

    blank = jnp.zeros((8, vecs), F32)
    for comp in range(3):
        for x in range(sx + (comp != 0)):
            for y in range(sy + (comp != 1)):
                base = at(comp, x, y)
                for t in range(0, stride, 8):
                    if t + 8 > sz:
                        ext_ref[base + t : base + t + 8] = blank
                if x < sx and y < sy:
                    col = vec_ref[comp, x, y]
                elif x == sx and y == sy:
                    col = xy_ref[...]
                elif x == sx:
                    row = ((comp - 1) * sy + y) * sz
                    col = x_ref[row : row + sz]
                else:
                    row = ((comp != 0) * sx + x) * sz
                    col = y_ref[row : row + sz]
                ext_ref[base : base + sz] = col
                if comp != 2:
                    if x == sx:
                        top = xz_ref[y : y + 1]
                    elif y == sy:
                        top = yz_ref[x : x + 1]
                    else:
                        row = (comp * sx + x) * sy + y
                        top = z_ref[row : row + 1]
                    ext_ref[base + sz : base + sz + 1] = top

    sub = lax.broadcasted_iota(jnp.int32, (8, vecs), 0)
    for i in range(counts[0]):
        for j in range(counts[1]):
            for k in range(counts[2]):
                e = (i * counts[1] + j) * counts[2] + k
                for comp in range(3):
                    shape = rows_of(comp)
                    columns = [(a, b) for a in range(shape[0]) for b in range(shape[1])]
                    for n in range(0, len(columns), 2):
                        (a, b), (a2, b2) = columns[n], columns[n + 1]
                        low = at(comp, 3 * i + a, 3 * j + b) + 3 * k
                        high = at(comp, 3 * i + a2, 3 * j + b2) + 3 * k - 4
                        tile = jnp.where(sub < 4, ext_ref[low : low + 8], ext_ref[high : high + 8])
                        row = STARTS[comp] + 4 * n
                        elem_ref[row : row + 8] = tile
                hi, lo = split(elem_ref[...])
                both = dot(hi_ref[e], jnp.concatenate([hi, lo], axis=1))
                out_ref[e, 8 : 8 + PADDED] = both[:, :vecs] + both[:, vecs:] + dot(lo_ref[e], hi)

    for comp in range(3):
        shape = rows_of(comp)
        for x in range(sx + (comp != 0)):
            for y in range(sy + (comp != 1)):
                for t in range(0, stride, 8):
                    total = None
                    for i in range(counts[0]):
                        a = x - 3 * i
                        if not 0 <= a < shape[0]:
                            continue
                        for j in range(counts[1]):
                            b = y - 3 * j
                            if not 0 <= b < shape[1]:
                                continue
                            row = 8 + STARTS[comp] + (a * shape[1] + b) * 4
                            for k in range(counts[2]):
                                first = 3 * k - t
                                if first >= 8 or first + shape[2] <= 0:
                                    continue
                                e = (i * counts[1] + j) * counts[2] + k
                                part = out_ref[e, row - first : row - first + 8]
                                keep = (sub >= first) & (sub < first + shape[2])
                                part = jnp.where(keep, part, 0.0)
                                total = part if total is None else total + part
                    if total is not None:
                        base = at(comp, x, y) - 8 + t
                        acc_ref[base : base + 8] = total

    length = [sz + 1, sz + 1, sz]
    for comp in range(3):
        for x in range(sx + (comp != 0)):
            for y in range(sy + (comp != 1)):
                base = at(comp, x, y) - 8
                res[comp][x, y] = acc_ref[base : base + length[comp]]

    put_faces(0, groups, sizes, res, msgs)


def shift(array, offset, dims):
    used = [d for d in range(3) if offset[d] % dims[d]]
    names = tuple(AXES[d] for d in used)
    lens = [dims[d] for d in used]
    pairs = []
    for src in np.ndindex(*lens):
        dst = tuple((s + offset[d]) % dims[d] for s, d in zip(src, used))
        pairs.append((int(np.ravel_multi_index(src, lens)), int(np.ravel_multi_index(dst, lens))))
    return lax.ppermute(array, names, pairs)


def on_device(dims, vectors, orient_flip, reluctivity, conductivity):
    counts = (orient_flip.shape[0], orient_flip.shape[1], orient_flip.shape[2] // ELEM_DOFS)
    elements = counts[0] * counts[1] * counts[2]
    sx, sy, sz = vectors.shape[1:4]
    sizes = (sx, sy, sz)
    vecs = vectors.shape[4]
    params = pltpu.CompilerParams(vmem_limit_bytes=16 * 2**20)

    def shape(*dims_now, dtype=F32):
        return jax.ShapeDtypeStruct(dims_now, dtype)

    table, weight, place = element_tables()
    first = PADDED + 8
    lanes = ELEM_DOFS * counts[2]
    width = max(6 * QPTS, -(-lanes // 128) * 128)
    const = np.zeros((first + PADDED * counts[2], width))
    const[:PADDED, : 6 * QPTS] = table.T
    const[PADDED, : 6 * QPTS] = weight
    for k in range(counts[2]):
        rows = slice(first + PADDED * k, first + PADDED * (k + 1))
        const[rows, ELEM_DOFS * k : ELEM_DOFS * (k + 1)] = place.T
    faces = pl.pallas_call(
        pack_kernel,
        out_shape=[
            shape(2 * sy * sz, vecs),
            shape(2 * sx * sz, vecs),
            shape(2 * sx * sy, vecs),
            shape(sz, vecs),
            shape(sy, vecs),
            shape(sx, vecs),
        ],
        compiler_params=params,
        name="pack",
    )(vectors)
    offsets = [(-1, 0, 0), (0, -1, 0), (0, 0, -1), (-1, -1, 0), (-1, 0, -1), (0, -1, -1)]
    halo = [shift(face, offset, dims) for face, offset in zip(faces, offsets)]
    mat_hi, mat_lo = pl.pallas_call(
        functools.partial(form_kernel, counts),
        out_shape=[shape(elements, PADDED, PADDED, dtype=BF16)] * 2,
        compiler_params=params,
        cost_estimate=pl.CostEstimate(
            flops=elements * PADDED * PADDED * 384 * 6, bytes_accessed=2000000, transcendentals=0
        ),
        name="form",
    )(jnp.asarray(const, F32), orient_flip, reluctivity, conductivity)

    grouped = [face_groups(axis, dims) for axis in range(3)]
    groups = [list(g.values()) for g in grouped]
    buffers = [[face_shape(axis, keys, sizes, vecs) for keys in groups[axis]] for axis in range(3)]
    stride = -(-(sz + 1) // 8) * 8
    rows = 3 * (sx + 1) * (sy + 1) * stride
    results = [shape(*region_shape(c, sizes), vecs) for c in range(3)]

    def send(axis, bufs):
        if "first" in grouped[axis]:
            n = dims[axis]
            swaps = []
            for odd in (0, 1):
                ends = [((i + odd) % n, (i + odd + 1) % n) for i in range(0, n, 2)]
                swaps.append(sorted(ends + [(b, a) for a, b in ends]))
            return [lax.ppermute(buf, AXES[axis], swap) for buf, swap in zip(bufs, swaps)]
        return [
            shift(buf, [by if d == axis else 0 for d in range(3)], dims)
            for buf, by in zip(bufs, grouped[axis])
        ]

    parts = pl.pallas_call(
        functools.partial(apply_kernel, counts, groups[0]),
        out_shape=results + buffers[0],
        scratch_shapes=[
            pltpu.VMEM((rows + 16, vecs), F32),
            pltpu.VMEM((PADDED, vecs), F32),
            pltpu.VMEM((elements, PADDED + 16, vecs), F32),
            pltpu.VMEM((rows, vecs), F32),
        ],
        compiler_params=params,
        cost_estimate=pl.CostEstimate(
            flops=elements * PADDED * PADDED * vecs * 6, bytes_accessed=3000000, transcendentals=0
        ),
        name="apply",
    )(vectors, *halo, mat_hi, mat_lo)
    for axis in range(2):
        parts = pl.pallas_call(
            functools.partial(middle_kernel, axis, groups[axis], groups[axis + 1], sizes),
            out_shape=results + buffers[axis + 1],
            compiler_params=params,
            name=f"middle_{axis}",
        )(*parts[:3], *send(axis, parts[3:]))
    out_z = shape(sx + 1, sz, sy + 1, vecs)
    outs = pl.pallas_call(
        functools.partial(last_kernel, 2, groups[2], sizes),
        out_shape=results[:2] + [out_z],
        compiler_params=params,
        name="last",
    )(*parts[:3], *send(2, parts[3:]))
    return outs[0], outs[1], jnp.swapaxes(outs[2], 1, 2)


def solution(mesh):
    dims = tuple(mesh.shape[axis] for axis in AXES)
    spec = P("gx", "gy", "gz")
    out = P("gx", "gy", "gz", None)
    return jax.shard_map(
        functools.partial(on_device, dims),
        mesh=mesh,
        in_specs=(P(None, "gx", "gy", "gz", None), spec, spec, spec),
        out_specs=(out, out, out),
        check_vma=False,
    )
```
